32 devices in a mesh: seq: 8 (over z, x), mem: 4 (over y, core).
Axes of the slice: x: 2, y: 2, z: 4, core: 2. Of those that a mesh axis runs over, the one named last changes fastest.
Arguments:
- queries: bfloat16 [4096, 2048], P(('seq', 'mem')), may hold values from -6 to 6
- keys: bfloat16 [4096, 2048], P(('seq', 'mem')), may hold values from -0.52734375 to 0.52734375
- values: bfloat16 [4096, 2048], P(('seq', 'mem')), may hold values from -6 to 6
- gamma: bfloat16 [4096, 16], P(('seq', 'mem')), as said below
- rate: bfloat16 [4, 16], replicated, as said below
- route_ids: int32 [4096, 2], P(('seq', 'mem')), may hold values from 0 to 3, all different within a row; in each aligned block of 128 rows (0 to 127, 128 to 255, ...) at most 96 rows name the same one
- route_weights: float32 [4096, 2], P(('seq', 'mem')), may hold values from 0.2 to 1
- norm_gain: float32 [2048], replicated, may hold values from 0.25 to 1.75
Outputs:
- mixed_out: bfloat16 [4096, 2048], P(('seq', 'mem'))
The draws below stay inside these ranges and needn't reach their ends.
Inputs may be any that keep to these rules, and one draw needn't show every extreme that they name: `route_ids`: each token names two different memories. The tokens of one device name one memory at most 96 times; some memory is named exactly 96 times by some device's tokens. `gamma`: Positive; from 0.5 up to 6144. `rate`: Positive; from 0.04 * 4 / 4096 up to 0.06.
All inputs are finite; a program needn't handle non-finite values.
Results may differ from the reference program's by a relative error of at most 0.0052.
Values may be sent and summed in bfloat16 or wider, within the bound.
A program may use at most 128 MiB of HBM per device.

```python
import math
import jax
import jax.numpy as jnp
import numpy as np
from jax import lax

TOK_DEV = 128
HEADS = 16
HD = 128
BLOCK = 128
MEMORY_COUNT = 4
C = 96
SEQUENCE_TOKENS = 4096
SLOTS = 3072
N_SEQ = 8
N_MEM = 4


def draw_gamma(key, part):
    key_base = jax.random.fold_in(key, 11)
    key_position = jax.random.fold_in(key, 12)
    key_size = jax.random.fold_in(key, 13)
    baseline_rows = jnp.exp(jax.random.uniform(key_base, (SEQUENCE_TOKENS, HEADS), jnp.float32, math.log(0.5), math.log(2.0)))
    spike_positions = jax.random.randint(key_position, (2 * MEMORY_COUNT,), 0, SEQUENCE_TOKENS)
    spike_mask = jnp.zeros((SEQUENCE_TOKENS,), jnp.float32).at[spike_positions].set(1.0)
    spike_magnitude = 4.4 * SEQUENCE_TOKENS / MEMORY_COUNT * jax.random.uniform(key_size, (SEQUENCE_TOKENS, 1), jnp.float32, 1.0, 1.2)
    return jnp.where(spike_mask[:, None] > 0.5, spike_magnitude, baseline_rows).astype(jnp.bfloat16)


def draw_rate(key, part):
    lowest = 0.05 * MEMORY_COUNT / SEQUENCE_TOKENS
    share = 0.5
    slow_pick = jax.random.uniform(jax.random.fold_in(key, 21), (MEMORY_COUNT, HEADS), jnp.float32) < share
    slow_rates = lowest * jnp.exp(jax.random.uniform(jax.random.fold_in(key, 22), (MEMORY_COUNT, HEADS), jnp.float32, 0.0, math.log(2.0)))
    fast_rates = jnp.exp(jax.random.uniform(jax.random.fold_in(key, 23), (MEMORY_COUNT, HEADS), jnp.float32, math.log(0.01), math.log(0.05)))
    return jnp.where(slow_pick, slow_rates, fast_rates).astype(jnp.bfloat16)


def steps_of(stream_key, shape, shards, low, largest):
    loudness = 1.0
    for axis_at, parts in shards:
        heights = jax.random.uniform(jax.random.fold_in(jax.random.fold_in(stream_key, 6), axis_at), (parts,), jnp.float32, low / len(shards), largest / len(shards))
        loudness = loudness * jnp.repeat(jnp.exp(heights), shape[axis_at] // parts).reshape((-1,) + (1,) * (len(shape) - 1 - axis_at))
    return loudness


def deal_out(own_key, own, number, rows, amount, top, bound, slope):
    sequence = jax.random.permutation(own_key, amount)
    packed, usual = load_shares(amount, rows * top, bound, slope, True), load_shares(amount, rows * top, bound, slope, False)
    places = jnp.arange(amount)

    def named(lengths, rotation):
        used = int((lengths > 0).sum())
        fixed = max(1, used // 4)
        moved = fixed + (places - fixed + rotation * (used - fixed)) % max(1, amount - fixed)
        return jnp.zeros((amount,), jnp.int32).at[sequence[jnp.where(places < fixed, places, moved)]].set(jnp.asarray(lengths, jnp.int32))

    lengths = jnp.where(number % 4 == 0, named(packed, number // 4), named(usual, number - number // 4 - 1))
    mixed = jax.random.permutation(jax.random.fold_in(own, 3), amount)
    giver, taker = mixed[0:amount // 2 * 2:2], mixed[1:amount // 2 * 2:2]
    room = jnp.minimum(lengths[giver] - 1, bound - lengths[taker]) // 2
    room = jnp.where((giver == sequence[0]) | (taker == sequence[0]) | (lengths[taker] == 0), 0, jnp.maximum(room, 0))
    moved = jax.random.randint(jax.random.fold_in(own, 4), (amount // 2,), 0, 1 << 20) % (room + 1)
    lengths = lengths.at[giver].add(-moved).at[taker].add(moved)
    items = jnp.searchsorted(jnp.cumsum(lengths), jnp.arange(rows * top), side="right").astype(jnp.int32)
    table = items.reshape(top, rows).T
    table = table[jax.random.permutation(jax.random.fold_in(own, 1), rows)]
    rotation = jax.random.randint(jax.random.fold_in(own, 2), (rows, 1), 0, top)
    return jnp.take_along_axis(table, (jnp.arange(top)[None, :] + rotation) % top, axis=1)


def load_shares(amount, total, limit, skew, full):
    portions = [(1 << 20) // math.isqrt(rank ** skew) + 1 for rank in range(1, amount + 1)]
    largest = limit if full else min(limit, max(-(-total // amount), total * portions[0] // sum(portions)))
    least = 1 if total - largest >= amount - 1 else 0
    given, rest = [largest] + [least] * (amount - 1), total - largest - least * (amount - 1)
    while rest > 0:
        movable = [i for i in range(1, amount) if given[i] < largest] or [i for i in range(1, amount) if given[i] < limit]
        mass, budget = sum([portions[i] for i in movable]), rest
        for i in movable:
            addition = min(limit - given[i], max(1, budget * portions[i] // mass), rest)
            given[i] = given[i] + addition
            rest = rest - addition
    return np.array(given)


def centred(stream_key, dims, scale, most, split=(), kind=jnp.bfloat16):
    values = scale * jax.random.normal(stream_key, dims, jnp.float32)
    if split:
        values = values * steps_of(stream_key, dims, split, -0.22, 0.18)
    return jnp.clip(values, -most, most).astype(kind)


def setup_inputs(seed: int = 0) -> dict:
    key_list = jax.random.split(jax.random.key(seed), 9)
    queries = centred(key_list[0], (SEQUENCE_TOKENS, HEADS * HD), 1.0, 6.0, ((0, 32),))
    keys = centred(key_list[1], (SEQUENCE_TOKENS, HEADS * HD), 0.088, 0.52734375, ((0, 32),))
    values = centred(key_list[2], (SEQUENCE_TOKENS, HEADS * HD), 1.0, 6.0, ((0, 32),))
    gamma = draw_gamma(jax.random.fold_in(key_list[8], 71), 0)
    rate = draw_rate(jax.random.fold_in(key_list[8], 71), 0)
    route_ids_keys = jax.random.split(jax.random.fold_in(key_list[5], 1), SEQUENCE_TOKENS // TOK_DEV)
    route_ids_turns = jax.random.permutation(jax.random.fold_in(key_list[5], 3), SEQUENCE_TOKENS // TOK_DEV)
    route_ids = jax.vmap(lambda own, number: deal_out(jax.random.fold_in(key_list[5], 2), own, number, TOK_DEV, MEMORY_COUNT, 2, C, 2))(route_ids_keys, route_ids_turns).reshape((SEQUENCE_TOKENS, 2))
    route_weights = jnp.clip(0.2 + 0.8 * jax.random.uniform(key_list[6], (SEQUENCE_TOKENS, 2), jnp.float32) ** steps_of(key_list[6], (SEQUENCE_TOKENS, 2), ((0, 32),), -0.2, 0.2), 0.2, 1.0)
    norm_gain = jnp.clip(1.0 + 0.15 * jax.random.normal(key_list[7], (HEADS * HD,), jnp.float32), 0.25, 1.75)
    return dict(queries=queries, keys=keys, values=values, gamma=gamma, rate=rate, route_ids=route_ids, route_weights=route_weights, norm_gain=norm_gain)


epsilon = 1e-06

def reference(queries, keys, values, gamma, rate, route_ids, route_weights, norm_gain):
    feat_count = HEADS * HD
    block_count = SLOTS // BLOCK
    device_ids = (jnp.arange(SEQUENCE_TOKENS, dtype=jnp.int32) // TOK_DEV).astype(jnp.int32)
    causal = (jnp.arange(BLOCK)[:, None] >= jnp.arange(BLOCK)[None, :])[:, :, None]
    highest = lax.Precision.HIGHEST

    def memory_pass(totals, memory):
        route_hits = (route_ids == memory).astype(jnp.int32)
        route_rank = (jnp.cumsum(route_hits.reshape(N_SEQ * N_MEM, TOK_DEV * 2), axis=1).astype(jnp.int32).reshape(SEQUENCE_TOKENS, 2) - 1).astype(jnp.int32)
        token_rank = lax.optimization_barrier(jnp.sum(route_hits * route_rank, axis=1)).astype(jnp.int32)
        routed = lax.optimization_barrier(jnp.sum(route_hits, axis=1))
        slot_ids = jnp.where(routed > 0, device_ids * C + token_rank, SLOTS).astype(jnp.int32)
        query_slots = jnp.zeros((SLOTS, feat_count), jnp.bfloat16).at[slot_ids].set(queries, mode='drop')
        key_slots = jnp.zeros((SLOTS, feat_count), jnp.bfloat16).at[slot_ids].set(keys, mode='drop')
        value_slots = jnp.zeros((SLOTS, feat_count), jnp.bfloat16).at[slot_ids].set(values, mode='drop')
        gamma_slots = jnp.zeros((SLOTS, HEADS), jnp.bfloat16).at[slot_ids].set(gamma, mode='drop')
        rate_now = rate[memory].astype(jnp.float32)

        def block_step(state_now, inputs_now):
            query_rows, key_rows, value_rows, gamma_rows = inputs_now
            query32 = query_rows.astype(jnp.float32)
            key32 = key_rows.astype(jnp.float32)
            value32 = value_rows.astype(jnp.float32)
            levels = jnp.cumsum(-rate_now[None, :] * gamma_rows.astype(jnp.float32), axis=0)
            spread_log = levels[:, None, :] - levels[None, :, :]
            decays = jnp.exp(jnp.where(causal, spread_log, -1e+30))
            scores = jnp.einsum('thd,shd->tsh', query32, key32, precision=highest)
            weights = lax.optimization_barrier((decays * scores).astype(jnp.bfloat16)).astype(jnp.float32)
            intra_out = jnp.einsum('tsh,she->the', weights, value32, precision=highest)
            inter_out = jnp.einsum('thd,hde->the', query32 * jnp.exp(levels)[:, :, None], state_now, precision=highest)
            raw_out = intra_out + inter_out
            normed = raw_out * lax.rsqrt(lax.optimization_barrier(jnp.mean(raw_out * raw_out, axis=-1, keepdims=True)) + epsilon)
            last_level = levels[-1]
            keyed_rows = lax.optimization_barrier((key32 * jnp.exp(last_level[None, :] - levels)[:, :, None]).astype(jnp.bfloat16)).astype(jnp.float32)
            state_next = jnp.exp(last_level)[:, None, None] * state_now + jnp.einsum('shd,she->hde', keyed_rows, value32, precision=highest)
            return (state_next, normed.astype(jnp.bfloat16))
        start_state = jnp.zeros((HEADS, HD, HD), jnp.float32)
        block_inputs = (query_slots.reshape(block_count, BLOCK, HEADS, HD), key_slots.reshape(block_count, BLOCK, HEADS, HD), value_slots.reshape(block_count, BLOCK, HEADS, HD), gamma_slots.reshape(block_count, BLOCK, HEADS))
        _, block_outs = lax.scan(block_step, start_state, block_inputs)
        block_outs = block_outs.reshape(SLOTS, feat_count)
        picked = jnp.take(block_outs, jnp.minimum(slot_ids, SLOTS - 1), axis=0).astype(jnp.float32)
        weight = lax.optimization_barrier(jnp.sum(jnp.where(route_hits > 0, route_weights, jnp.float32(0.0)), axis=1))
        return (totals + weight[:, None] * picked, None)
    totals, _ = lax.scan(memory_pass, jnp.zeros((SEQUENCE_TOKENS, feat_count), jnp.float32), jnp.arange(N_MEM, dtype=jnp.int32))
    return (totals * norm_gain[None, :]).astype(jnp.bfloat16)
```

```python
import functools

import jax
import jax.numpy as jnp
from jax import lax
from jax.experimental import pallas as pl
from jax.experimental.pallas import tpu as pltpu
from jax.sharding import PartitionSpec as P

EPSILON = 1e-06
FAR = 1e30
F32 = jnp.float32
BF16 = jnp.bfloat16


def dot(a, b, dims=((1,), (0,))):
    return lax.dot_general(a, b, (dims, ((), ())), preferred_element_type=F32)


def kernel(n, seqs, hl, mems, pair, q_ref, k_ref, v_ref, aux_ref, rate_ref, gain_ref, out_ref,
           qbuf, kbuf, vbuf, auxb, lrm, kew, adec, atot, apart, cols, pbuf, u32, ubf, upart,
           esend, erecv, sgrp, raw, outb,
           aux_s, aux_r, tok_s, tok_r, a_s, a_r, u_s, u_r, e_s, e_r, o_s, o_r):
    me = lax.axis_index("mem")
    pos = lax.axis_index("seq")
    tok = q_ref.shape[0]
    hd = qbuf.shape[-1]
    inner = lax.rem(pos, pair)
    even = inner == 0
    mate = pos + 1 - 2 * inner
    first = pos < pair
    last = pos + pair >= seqs
    rank = lax.div(pos, pair)

    def peer(step):
        return lax.rem(me + step, n)

    def lanes(head):
        return pl.ds(pl.multiple_of(head * hd, hd), hd)

    def token_copy(t, h, dst, slot):
        src, buf = ((k_ref, kbuf), (v_ref, vbuf), (q_ref, qbuf))[t]
        return pltpu.make_async_remote_copy(
            src_ref=src.at[:, lanes(dst * hl + h)], dst_ref=buf.at[slot, h],
            send_sem=tok_s.at[t, h, dst], recv_sem=tok_r.at[t, h, slot],
            device_id={"mem": dst}, device_id_type=pl.DeviceIdType.MESH)

    def aux_copy(dst, slot):
        return pltpu.make_async_remote_copy(
            src_ref=aux_ref, dst_ref=auxb.at[slot], send_sem=aux_s.at[dst], recv_sem=aux_r.at[slot],
            device_id={"mem": dst}, device_id_type=pl.DeviceIdType.MESH)

    def a_copy():
        return pltpu.make_async_remote_copy(
            src_ref=atot, dst_ref=apart, send_sem=a_s, recv_sem=a_r,
            device_id={"seq": mate}, device_id_type=pl.DeviceIdType.MESH)

    def u_copy(h):
        return pltpu.make_async_remote_copy(
            src_ref=ubf.at[h], dst_ref=upart.at[h], send_sem=u_s.at[h], recv_sem=u_r.at[h],
            device_id={"seq": mate}, device_id_type=pl.DeviceIdType.MESH)

    def e_copy(h):
        return pltpu.make_async_remote_copy(
            src_ref=esend.at[h], dst_ref=erecv.at[h], send_sem=e_s.at[h], recv_sem=e_r.at[h],
            device_id={"seq": lax.rem(pos + pair, seqs)}, device_id_type=pl.DeviceIdType.MESH)

    def out_copy(h, dst, slot):
        return pltpu.make_async_remote_copy(
            src_ref=outb.at[h, dst], dst_ref=out_ref.at[:, lanes(slot * hl + h)],
            send_sem=o_s.at[h, dst], recv_sem=o_r.at[h, slot],
            device_id={"mem": dst}, device_id_type=pl.DeviceIdType.MESH)

    barrier = pltpu.get_barrier_semaphore()

    def greet(**where):
        pl.semaphore_signal(barrier, inc=1, device_id=where, device_id_type=pl.DeviceIdType.MESH)

    for step in range(1, n):
        greet(mem=peer(step))
    greet(seq=mate)

    @pl.when(jnp.logical_not(first))
    def _():
        greet(seq=pos - pair)

    @pl.when(jnp.logical_not(last))
    def _():
        greet(seq=pos + pair)

    pl.semaphore_wait(barrier, n + jnp.minimum(rank, 1) + jnp.minimum(seqs // pair - 1 - rank, 1))

    for step in range(1, n):
        aux_copy(peer(step), me).start()
    for h in range(hl):
        for t in (0, 1):
            for step in range(1, n):
                token_copy(t, h, peer(step), me).start()
    for h in range(hl):
        for step in range(1, n):
            token_copy(2, h, peer(step), me).start()

    auxb[me] = aux_ref[...]
    for h in range(hl):
        kbuf[me, h] = k_ref[:, lanes(me * hl + h)]
        vbuf[me, h] = v_ref[:, lanes(me * hl + h)]
        qbuf[me, h] = q_ref[:, lanes(me * hl + h)]

    row_at = lax.broadcasted_iota(jnp.int32, (tok, tok), 0)
    col_at = lax.broadcasted_iota(jnp.int32, (tok, tok), 1)
    upper = (row_at <= col_at).astype(BF16)
    heads = hl * n
    for step in range(1, n):
        aux_copy(peer(step), peer(step)).wait_recv()

    rates = rate_ref[pl.ds(pl.multiple_of(me * hl * mems, hl * mems), hl * mems), :]
    total = jnp.zeros((hl * mems, tok), F32)
    mem_at = lax.broadcasted_iota(jnp.int32, (mems, tok), 0).astype(F32)
    for j in range(n):
        ids = [auxb[j, heads + r:heads + r + 1, :] for r in (0, 1)]
        wts = [auxb[j, heads + 2 + r:heads + 3 + r, :] for r in (0, 1)]
        hit = [ids[r] == mem_at for r in (0, 1)]
        mask = jnp.logical_or(hit[0], hit[1])
        gam = [auxb[j, pl.ds(me * hl + h, 1), :] for h in range(hl)]
        picked = jnp.concatenate([jnp.where(mask, g, 0.0) for g in gam], axis=0)
        level = -rates * dot(picked.astype(BF16), upper)
        here = jnp.concatenate([jnp.where(mask, 1.0, 0.0)] * hl, axis=0) > 0.5
        end = jnp.broadcast_to(level[:, tok - 1:tok], level.shape)
        lrm[j] = jnp.where(here, level, FAR)
        kew[j] = jnp.where(here, jnp.exp(end - level), 0.0)
        adec[j] = jnp.exp(end)
        for h in range(hl):
            own = level[h * mems:(h + 1) * mems]
            ahead = own + total[h * mems:(h + 1) * mems]
            rows = [jnp.sum(jnp.where(hit[r], own, 0.0), axis=0, keepdims=True) for r in (0, 1)]
            rows += [jnp.sum(jnp.where(hit[r], ahead, 0.0), axis=0, keepdims=True) for r in (0, 1)]
            cols[j, h] = jnp.concatenate(rows + ids + wts, axis=0).T
        total = total + end
    atot[...] = jnp.exp(total)
    a_copy().start()

    def update(h):
        for j in range(n):
            @pl.when(me != j)
            def _():
                token_copy(0, h, j, j).wait_recv()
                token_copy(1, h, j, j).wait_recv()
        state = jnp.zeros((mems * hd, hd), F32)
        for j in range(n):
            turned = kbuf[j, h].astype(F32).T
            keyed = jnp.concatenate(
                [(turned * kew[j, pl.ds(h * mems + m, 1), :]).astype(BF16) for m in range(mems)], axis=0)
            fresh = dot(keyed, vbuf[j, h])
            if j > 0:
                pbuf[h, j] = state.astype(BF16)
                state = jnp.concatenate(
                    [adec[j, pl.ds(h * mems + m, 1), :] * state[m * hd:(m + 1) * hd] for m in range(mems)],
                    axis=0) + fresh
            else:
                state = fresh
        u32[h] = state
        ubf[h] = state.astype(BF16)
        u_copy(h).start()

    def select(ident, parts):
        got = parts[0]
        for m in range(1, mems):
            got = jnp.where(ident == float(m), parts[m], got)
        return got

    def intra(h):
        for j in range(n):
            @pl.when(me != j)
            def _():
                token_copy(2, h, j, j).wait_recv()
        causal = row_at >= col_at
        for j in range(n):
            query, value = qbuf[j, h], vbuf[j, h]
            score = dot(query, kbuf[j, h], ((1,), (1,)))
            col = cols[j, h]
            rows = [lrm[j, pl.ds(h * mems + m, 1), :] for m in range(mems)]
            weights = []
            for r in (0, 1):
                spread = col[:, r:r + 1] - select(col[:, 4 + r:5 + r], rows)
                decay = jnp.exp(jnp.where(causal, spread, -FAR))
                weights.append((decay * score).astype(BF16))
            inside = dot(jnp.concatenate(weights, axis=0), value)
            if j > 0:
                before = [dot(query, pbuf[h, j, m * hd:(m + 1) * hd, :]) for m in range(mems)]
            for r in (0, 1):
                part = inside[r * tok:(r + 1) * tok]
                if j > 0:
                    part = part + jnp.exp(col[:, r:r + 1]) * select(col[:, 4 + r:5 + r], before)
                raw[h, j, r] = part

    def relay(h, carry):
        @pl.when(h == 0)
        def _():
            a_copy().wait_recv()

        u_copy(h).wait_recv()

        @pl.when(first)
        def _():
            erecv[h] = jnp.zeros(erecv.shape[1:], BF16)

        @pl.when(jnp.logical_not(first))
        def _():
            e_copy(h).wait_recv()

        @pl.when(jnp.logical_not(last))
        def _():
            for m in range(mems):
                at = slice(m * hd, (m + 1) * hd)
                mine, other = atot[pl.ds(h * mems + m, 1), :], apart[pl.ds(h * mems + m, 1), :]
                own = jnp.where(even, other, 1.0) * u32[h, at, :]
                both = own + jnp.where(even, 1.0, mine) * upart[h, at, :].astype(F32)
                esend[h, at, :] = (both + mine * other * erecv[h, at, :].astype(F32)).astype(BF16)
            e_copy(h).start()

        @pl.when(even)
        def _():
            sgrp[h] = erecv[h]

        @pl.when(jnp.logical_not(even))
        def _():
            for m in range(mems):
                at = slice(m * hd, (m + 1) * hd)
                other = apart[pl.ds(h * mems + m, 1), :]
                sgrp[h, at, :] = (other * erecv[h, at, :].astype(F32) + upart[h, at, :].astype(F32)).astype(BF16)

        return carry

    def due(phase):
        return jnp.clip(phase - 1 - 2 * rank, 0, hl)

    def phase_step(phase, carry):
        @pl.when(phase < hl)
        def _():
            update(phase)

        @pl.when(phase >= hl)
        def _():
            intra(phase - hl)

        lax.fori_loop(due(phase), due(phase + 1), relay, 0)
        return carry

    lax.fori_loop(0, 2 * hl, phase_step, 0)
    relayed = due(2 * hl)

    def finish(h, carry):
        @pl.when(h >= relayed)
        def _():
            relay(h, 0)

        gain = gain_ref[pl.ds(me * hl + h, 1), :]
        for j in range(n):
            query, col = qbuf[j, h], cols[j, h]
            before = [dot(query, sgrp[h, m * hd:(m + 1) * hd, :]) for m in range(mems)]
            mixed = jnp.zeros((tok, hd), F32)
            for r in (0, 1):
                part = raw[h, j, r] + jnp.exp(col[:, 2 + r:3 + r]) * select(col[:, 4 + r:5 + r], before)
                scale = lax.rsqrt(jnp.mean(part * part, axis=-1, keepdims=True) + EPSILON)
                mixed = mixed + col[:, 6 + r:7 + r] * (part * scale).astype(BF16).astype(F32)
            done = (mixed * gain).astype(BF16)

            @pl.when(me == j)
            def _():
                out_ref[:, lanes(me * hl + h)] = done

            @pl.when(me != j)
            def _():
                outb[h, j] = done
                out_copy(h, j, me).start()
        return carry

    lax.fori_loop(0, hl, finish, 0)

    for step in range(1, n):
        there = peer(step)
        aux_copy(there, me).wait_send()
        for h in range(hl):
            for t in range(3):
                token_copy(t, h, there, me).wait_send()
            out_copy(h, there, me).wait_send()
            out_copy(h, there, there).wait_recv()
    a_copy().wait_send()
    for h in range(hl):
        u_copy(h).wait_send()

        @pl.when(jnp.logical_not(last))
        def _():
            e_copy(h).wait_send()


def body(n, seqs, queries, keys, values, gamma, rate, route_ids, route_weights, norm_gain):
    tok, feats = queries.shape
    heads = gamma.shape[1]
    mems = rate.shape[0]
    hd = feats // heads
    hl = heads // n
    pair = 2
    aux = jnp.concatenate([gamma.astype(F32), route_ids.astype(F32), route_weights], axis=1).T
    aux = jnp.pad(aux, ((0, -aux.shape[0] % 8), (0, 0)))
    rates = jnp.broadcast_to(rate.astype(F32).T.reshape(heads * mems, 1), (heads * mems, tok))
    gain = norm_gain.reshape(heads, hd)
    vm = pltpu.VMEM
    dma = pltpu.SemaphoreType.DMA
    rows = hl * mems
    scratch = [
        vm((n, hl, tok, hd), BF16), vm((n, hl, tok, hd), BF16), vm((n, hl, tok, hd), BF16),
        vm((n,) + aux.shape, F32),
        vm((n, rows, tok), F32), vm((n, rows, tok), F32), vm((n, rows, tok), F32),
        vm((rows, tok), F32), vm((rows, tok), F32),
        vm((n, hl, tok, 8), F32),
        vm((hl, n, mems * hd, hd), BF16),
        vm((hl, mems * hd, hd), F32), vm((hl, mems * hd, hd), BF16), vm((hl, mems * hd, hd), BF16),
        vm((hl, mems * hd, hd), BF16), vm((hl, mems * hd, hd), BF16), vm((hl, mems * hd, hd), BF16),
        vm((hl, n, 2, tok, hd), F32),
        vm((hl, n, tok, hd), BF16),
        dma((n,)), dma((n,)), dma((3, hl, n)), dma((3, hl, n)), dma, dma,
        dma((hl,)), dma((hl,)), dma((hl,)), dma((hl,)), dma((hl, n)), dma((hl, n)),
    ]
    spec = pl.BlockSpec(memory_space=pltpu.VMEM)
    return pl.pallas_call(
        functools.partial(kernel, n, seqs, hl, mems, pair),
        out_shape=jax.ShapeDtypeStruct((tok, feats), BF16),
        in_specs=[spec] * 6,
        out_specs=spec,
        scratch_shapes=scratch,
        compiler_params=pltpu.CompilerParams(
            collective_id=0, has_side_effects=True, vmem_limit_bytes=60 * 1024 * 1024),
    )(queries, keys, values, aux, rates, gain)


def solution(mesh):
    rows = P(("seq", "mem"), None)
    in_specs = (rows, rows, rows, rows, P(), rows, rows, P())
    run = functools.partial(body, mesh.shape["mem"], mesh.shape["seq"])
    return jax.shard_map(run, mesh=mesh, in_specs=in_specs, out_specs=rows, check_vma=False)
```

```python
import functools

import jax
import jax.numpy as jnp
from jax import lax
from jax.experimental import pallas as pl
from jax.experimental.pallas import tpu as pltpu
from jax.sharding import PartitionSpec as P

EPSILON = 1e-06
FAR = 1e30
F32 = jnp.float32
BF16 = jnp.bfloat16


def dot(a, b, dims=((1,), (0,))):
    return lax.dot_general(a, b, (dims, ((), ())), preferred_element_type=F32)


def kernel(n, seqs, hl, mems, pair, q_ref, k_ref, v_ref, gamma_ref, rate_ref,
           ids_ref, wts_ref, gain_ref, out_ref, aux_ref,
           qbuf, kbuf, vbuf, auxb, lrm, kew, adec, atot, apart, cols, pbuf, u32, ubf, upart,
           esend, erecv, sgrp, raw, outb,
           aux_s, aux_r, tok_s, tok_r, a_s, a_r, u_s, u_r, e_s, e_r, o_s, o_r):
    me = lax.axis_index("mem")
    pos = lax.axis_index("seq")
    tok = q_ref.shape[0]
    hd = qbuf.shape[-1]
    inner = lax.rem(pos, pair)
    even = inner == 0
    mate = pos + 1 - 2 * inner
    first = pos < pair
    last = pos + pair >= seqs
    rank = lax.div(pos, pair)

    def peer(step):
        return lax.rem(me + step, n)

    def lanes(head):
        return pl.ds(pl.multiple_of(head * hd, hd), hd)

    def token_copy(t, h, dst, slot):
        src, buf = ((k_ref, kbuf), (v_ref, vbuf), (q_ref, qbuf))[t]
        return pltpu.make_async_remote_copy(
            src_ref=src.at[:, lanes(dst * hl + h)], dst_ref=buf.at[slot, h],
            send_sem=tok_s.at[t, h, dst], recv_sem=tok_r.at[t, h, slot],
            device_id={"mem": dst}, device_id_type=pl.DeviceIdType.MESH)

    def aux_copy(dst, slot):
        return pltpu.make_async_remote_copy(
            src_ref=aux_ref, dst_ref=auxb.at[slot], send_sem=aux_s.at[dst], recv_sem=aux_r.at[slot],
            device_id={"mem": dst}, device_id_type=pl.DeviceIdType.MESH)

    def a_copy():
        return pltpu.make_async_remote_copy(
            src_ref=atot, dst_ref=apart, send_sem=a_s, recv_sem=a_r,
            device_id={"seq": mate}, device_id_type=pl.DeviceIdType.MESH)

    def u_copy(h, m):
        return pltpu.make_async_remote_copy(
            src_ref=ubf.at[h, m], dst_ref=upart.at[h, m], send_sem=u_s.at[h, m], recv_sem=u_r.at[h, m],
            device_id={"seq": mate}, device_id_type=pl.DeviceIdType.MESH)

    def e_copy(h, m):
        return pltpu.make_async_remote_copy(
            src_ref=esend.at[h, m], dst_ref=erecv.at[h, m], send_sem=e_s.at[h, m], recv_sem=e_r.at[h, m],
            device_id={"seq": lax.rem(pos + pair, seqs)}, device_id_type=pl.DeviceIdType.MESH)

    def out_copy(h, dst, slot):
        return pltpu.make_async_remote_copy(
            src_ref=outb.at[h, dst], dst_ref=out_ref.at[:, lanes(slot * hl + h)],
            send_sem=o_s.at[h, dst], recv_sem=o_r.at[h, slot],
            device_id={"mem": dst}, device_id_type=pl.DeviceIdType.MESH)

    barrier = pltpu.get_barrier_semaphore()

    def greet(**where):
        pl.semaphore_signal(barrier, inc=1, device_id=where, device_id_type=pl.DeviceIdType.MESH)

    for step in range(1, n):
        greet(mem=peer(step))
    greet(seq=mate)

    @pl.when(jnp.logical_not(first))
    def _():
        greet(seq=pos - pair)

    @pl.when(jnp.logical_not(last))
    def _():
        greet(seq=pos + pair)

    row_at = lax.broadcasted_iota(jnp.int32, (tok, tok), 0)
    col_at = lax.broadcasted_iota(jnp.int32, (tok, tok), 1)
    heads = hl * n
    eye = (row_at == col_at).astype(BF16)
    aux_ref[0:heads, :] = dot(gamma_ref[...], eye, ((0,), (0,)))
    aux_ref[heads:heads + 2, :] = dot(ids_ref[...].astype(BF16), eye, ((0,), (0,)))
    aux_ref[heads + 2:heads + 4, :] = lax.dot_general(
        wts_ref[...], eye.astype(F32), (((0,), (0,)), ((), ())),
        precision=lax.Precision.HIGHEST, preferred_element_type=F32)
    aux_ref[heads + 4:, :] = jnp.zeros((aux_ref.shape[0] - heads - 4, tok), F32)

    pl.semaphore_wait(barrier, n + jnp.minimum(rank, 1) + jnp.minimum(seqs // pair - 1 - rank, 1))

    for step in range(1, n):
        aux_copy(peer(step), me).start()
    for h in range(hl):
        for t in (0, 1):
            for step in range(1, n):
                token_copy(t, h, peer(step), me).start()
    for h in range(hl):
        for step in range(1, n):
            token_copy(2, h, peer(step), me).start()

    auxb[me] = aux_ref[...]
    for h in range(hl):
        kbuf[me, h] = k_ref[:, lanes(me * hl + h)]
        vbuf[me, h] = v_ref[:, lanes(me * hl + h)]
        qbuf[me, h] = q_ref[:, lanes(me * hl + h)]

    upper = (row_at <= col_at).astype(BF16)
    for step in range(1, n):
        aux_copy(peer(step), peer(step)).wait_recv()

    table = rate_ref[...].astype(F32)
    head_at = lax.broadcasted_iota(jnp.int32, table.shape, 1)
    rates = jnp.concatenate(
        [jnp.sum(jnp.where(head_at == me * hl + h, table, 0.0), axis=1, keepdims=True) for h in range(hl)], axis=0)
    total = jnp.zeros((hl * mems, tok), F32)
    mem_at = lax.broadcasted_iota(jnp.int32, (mems, tok), 0).astype(F32)
    for j in range(n):
        ids = [auxb[j, heads + r:heads + r + 1, :] for r in (0, 1)]
        wts = [auxb[j, heads + 2 + r:heads + 3 + r, :] for r in (0, 1)]
        hit = [ids[r] == mem_at for r in (0, 1)]
        mask = jnp.logical_or(hit[0], hit[1])
        gam = [auxb[j, pl.ds(me * hl + h, 1), :] for h in range(hl)]
        picked = jnp.concatenate([jnp.where(mask, g, 0.0) for g in gam], axis=0)
        level = -rates * dot(picked.astype(BF16), upper)
        here = jnp.concatenate([jnp.where(mask, 1.0, 0.0)] * hl, axis=0) > 0.5
        end = jnp.broadcast_to(level[:, tok - 1:tok], level.shape)
        lrm[j] = jnp.where(here, level, FAR)
        kew[j] = jnp.where(here, jnp.exp(end - level), 0.0)
        adec[j] = jnp.exp(end)
        for h in range(hl):
            own = level[h * mems:(h + 1) * mems]
            ahead = own + total[h * mems:(h + 1) * mems]
            rows = [jnp.sum(jnp.where(hit[r], own, 0.0), axis=0, keepdims=True) for r in (0, 1)]
            rows += [jnp.sum(jnp.where(hit[r], ahead, 0.0), axis=0, keepdims=True) for r in (0, 1)]
            cols[j, h] = jnp.concatenate(rows + ids + wts, axis=0).T
        total = total + end
    atot[...] = jnp.exp(total)
    a_copy().start()

    def update(h):
        for j in range(n):
            @pl.when(me != j)
            def _():
                token_copy(0, h, j, j).wait_recv()
                token_copy(1, h, j, j).wait_recv()
        state = jnp.zeros((mems * hd, hd), F32)
        for j in range(n):
            turned = kbuf[j, h].astype(F32).T
            keyed = jnp.concatenate(
                [(turned * kew[j, pl.ds(h * mems + m, 1), :]).astype(BF16) for m in range(mems)], axis=0)
            fresh = dot(keyed, vbuf[j, h])
            if j > 0:
                pbuf[h, j] = state.astype(BF16)
                state = jnp.concatenate(
                    [adec[j, pl.ds(h * mems + m, 1), :] * state[m * hd:(m + 1) * hd] for m in range(mems)],
                    axis=0) + fresh
            else:
                state = fresh
        for m in range(mems):
            u32[h, m] = state[m * hd:(m + 1) * hd]
            ubf[h, m] = state[m * hd:(m + 1) * hd].astype(BF16)
            u_copy(h, m).start()

    def select(ident, parts):
        got = parts[0]
        for m in range(1, mems):
            got = jnp.where(ident == float(m), parts[m], got)
        return got

    def intra(h):
        for j in range(n):
            @pl.when(me != j)
            def _():
                token_copy(2, h, j, j).wait_recv()
        causal = row_at >= col_at
        for j in range(n):
            query, value = qbuf[j, h], vbuf[j, h]
            score = dot(query, kbuf[j, h], ((1,), (1,)))
            col = cols[j, h]
            rows = [lrm[j, pl.ds(h * mems + m, 1), :] for m in range(mems)]
            weights = []
            for r in (0, 1):
                spread = col[:, r:r + 1] - select(col[:, 4 + r:5 + r], rows)
                decay = jnp.exp(jnp.where(causal, spread, -FAR))
                weights.append((decay * score).astype(BF16))
            inside = dot(jnp.concatenate(weights, axis=0), value)
            if j > 0:
                before = [dot(query, pbuf[h, j, m * hd:(m + 1) * hd, :]) for m in range(mems)]
            for r in (0, 1):
                part = inside[r * tok:(r + 1) * tok]
                if j > 0:
                    part = part + jnp.exp(col[:, r:r + 1]) * select(col[:, 4 + r:5 + r], before)
                raw[h, j, r] = part

    def relay(h, carry):
        @pl.when(h == 0)
        def _():
            a_copy().wait_recv()

        def one(m, inside):
            mine, other = atot[pl.ds(h * mems + m, 1), :], apart[pl.ds(h * mems + m, 1), :]
            u_copy(h, m).wait_recv()

            @pl.when(first)
            def _():
                erecv[h, m] = jnp.zeros((hd, hd), BF16)

            @pl.when(jnp.logical_not(first))
            def _():
                e_copy(h, m).wait_recv()

            @pl.when(jnp.logical_not(last))
            def _():
                both = jnp.where(even, other, 1.0) * u32[h, m]
                both = both + jnp.where(even, 1.0, mine) * upart[h, m].astype(F32)
                esend[h, m] = (both + mine * other * erecv[h, m].astype(F32)).astype(BF16)
                e_copy(h, m).start()

            @pl.when(even)
            def _():
                sgrp[h, m] = erecv[h, m]

            @pl.when(jnp.logical_not(even))
            def _():
                sgrp[h, m] = (other * erecv[h, m].astype(F32) + upart[h, m].astype(F32)).astype(BF16)

            return inside

        lax.fori_loop(0, mems, one, 0)
        return carry

    def finish(h):
        gain = gain_ref[:, lanes(me * hl + h)]
        for j in range(n):
            query, col = qbuf[j, h], cols[j, h]
            before = [dot(query, sgrp[h, m]) for m in range(mems)]
            mixed = jnp.zeros((tok, hd), F32)
            for r in (0, 1):
                part = raw[h, j, r] + jnp.exp(col[:, 2 + r:3 + r]) * select(col[:, 4 + r:5 + r], before)
                scale = lax.rsqrt(jnp.mean(part * part, axis=-1, keepdims=True) + EPSILON)
                mixed = mixed + col[:, 6 + r:7 + r] * (part * scale).astype(BF16).astype(F32)
            done = (mixed * gain).astype(BF16)

            @pl.when(me == j)
            def _():
                out_ref[:, lanes(me * hl + h)] = done

            @pl.when(me != j)
            def _():
                outb[h, j] = done
                out_copy(h, j, me).start()

    def due(phase):
        return jnp.clip(jnp.maximum(phase - 1 - 2 * rank, phase - 2 * hl + 1), 0, hl)

    def phase_step(phase, carry):
        @pl.when(phase < hl)
        def _():
            update(phase)

        @pl.when(jnp.logical_and(phase >= hl, phase < 2 * hl))
        def _():
            intra(phase - hl)

        @pl.when(phase >= 2 * hl)
        def _():
            finish(phase - 2 * hl)

        lax.fori_loop(due(phase), due(phase + 1), relay, 0)
        return carry

    lax.fori_loop(0, 3 * hl, phase_step, 0)

    for step in range(1, n):
        there = peer(step)
        aux_copy(there, me).wait_send()
        for h in range(hl):
            for t in range(3):
                token_copy(t, h, there, me).wait_send()
            out_copy(h, there, me).wait_send()
            out_copy(h, there, there).wait_recv()
    a_copy().wait_send()
    for h in range(hl):
        for m in range(mems):
            u_copy(h, m).wait_send()

            @pl.when(jnp.logical_not(last))
            def _():
                e_copy(h, m).wait_send()


def body(n, seqs, queries, keys, values, gamma, rate, route_ids, route_weights, norm_gain):
    tok, feats = queries.shape
    heads = gamma.shape[1]
    mems = rate.shape[0]
    hd = feats // heads
    hl = heads // n
    pair = 2
    aux_rows = -(-(heads + 4) // 8) * 8
    vm = pltpu.VMEM
    dma = pltpu.SemaphoreType.DMA
    rows = hl * mems
    scratch = [
        vm((aux_rows, tok), F32),
        vm((n, hl, tok, hd), BF16), vm((n, hl, tok, hd), BF16), vm((n, hl, tok, hd), BF16),
        vm((n, aux_rows, tok), F32),
        vm((n, rows, tok), F32), vm((n, rows, tok), F32), vm((n, rows, tok), F32),
        vm((rows, tok), F32), vm((rows, tok), F32),
        vm((n, hl, tok, 8), F32),
        vm((hl, n, mems * hd, hd), BF16),
        vm((hl, mems, hd, hd), F32), vm((hl, mems, hd, hd), BF16), vm((hl, mems, hd, hd), BF16),
        vm((hl, mems, hd, hd), BF16), vm((hl, mems, hd, hd), BF16), vm((hl, mems, hd, hd), BF16),
        vm((hl, n, 2, tok, hd), F32),
        vm((hl, n, tok, hd), BF16),
        dma((n,)), dma((n,)), dma((3, hl, n)), dma((3, hl, n)), dma, dma,
        dma((hl, mems)), dma((hl, mems)), dma((hl, mems)), dma((hl, mems)), dma((hl, n)), dma((hl, n)),
    ]
    spec = pl.BlockSpec(memory_space=pltpu.VMEM)
    return pl.pallas_call(
        functools.partial(kernel, n, seqs, hl, mems, pair),
        out_shape=jax.ShapeDtypeStruct((tok, feats), BF16),
        in_specs=[spec] * 8,
        out_specs=spec,
        scratch_shapes=scratch,
        compiler_params=pltpu.CompilerParams(
            collective_id=0, has_side_effects=True, vmem_limit_bytes=60 * 1024 * 1024),
    )(queries, keys, values, gamma, rate, route_ids, route_weights, norm_gain.reshape(1, feats))


def solution(mesh):
    rows = P(("seq", "mem"), None)
    in_specs = (rows, rows, rows, rows, P(), rows, rows, P())
    run = functools.partial(body, mesh.shape["mem"], mesh.shape["seq"])
    return jax.shard_map(run, mesh=mesh, in_specs=in_specs, out_specs=rows, check_vma=False)
```
